32 devices in a mesh: dp: 8 (over z, x), shard: 4 (over y, core).
Axes of the slice: x: 2, y: 2, z: 4, core: 2. Of those that a mesh axis runs over, the one named last changes fastest.
Arguments:
- code_ids: int32 [16384, 4], P(('dp', 'shard')), may hold values from 0 to 2047
- target_ids: int32 [16384, 4], P(('dp', 'shard')), may hold values from 0 to 2047
- valid_mask: int32 [16384, 4], P(('dp', 'shard')), may hold values 0 or 1
- clip_weight: int32 [32], P(('dp', 'shard')), may hold values from 0 to 3
- text_states: bfloat16 [2048, 1024], P(('dp', 'shard')), may hold values from -6 to 6
- layer_master: float32 [16384, 1024], P('shard'), may hold values from -0.5 to 0.5
- layer_first: float32 [16384, 1024], P('shard'), may hold values from -0.00015258789 to 0.00015258789
- layer_second: float32 [16384, 1024], P('shard'), may hold values from 1e-10 to 1e-09
- norm_master: float32 [8, 1024], P(None, 'shard'), may hold values from -1.2 to 1.45
- norm_first: float32 [8, 1024], P(None, 'shard'), may hold values from -0.00015258789 to 0.00015258789
- norm_second: float32 [8, 1024], P(None, 'shard'), may hold values from 1e-10 to 1e-09
- table_master: float32 [2, 8192, 1024], P(None, ('dp', 'shard')), may hold values from -2 to 2
- table_first: float32 [2, 8192, 1024], P(None, ('dp', 'shard')), may hold values from -0.00015258789 to 0.00015258789
- table_second: float32 [2, 8192, 1024], P(None, ('dp', 'shard')), may hold values from 1e-10 to 1e-09
- step_count: int32 [1], replicated, may hold values from 1 to 20
Outputs:
- loss: float32 [1], replicated
- grad_norm: float32 [1], replicated
- new_layer: float32 [16384, 1024], P('shard')
- new_layer_first: float32 [16384, 1024], P('shard')
- new_layer_second: float32 [16384, 1024], P('shard')
- new_norm: float32 [8, 1024], P(None, 'shard')
- new_norm_first: float32 [8, 1024], P(None, 'shard')
- new_norm_second: float32 [8, 1024], P(None, 'shard')
- new_table: float32 [2, 8192, 1024], P(None, ('dp', 'shard'))
- new_table_first: float32 [2, 8192, 1024], P(None, ('dp', 'shard'))
- new_table_second: float32 [2, 8192, 1024], P(None, ('dp', 'shard'))
The draws below stay inside these ranges and needn't reach their ends.
Inputs may be any that keep to these rules, and one draw needn't show every extreme that they name: `clip_weight`: 0 marks a pad clip.
All inputs are finite; a program needn't handle non-finite values. No bound on the sum of `valid_mask` on one device may be relied on, other than what follows from the above.
Results may differ from the reference program's by a relative error of at most 0.0015.
The reference program's roundings to bfloat16 on the way count: a program that leaves them out, or rounds other values in their place, can miss the bound.
Values may be sent and summed in bfloat16 or wider, within the bound.
A program may use at most 576 MiB of HBM per device.

```python
import math
import jax
import jax.numpy as jnp
import numpy as np
from jax import lax

D = 1024
HEADS = 16
HEAD = 64
FF = 4096
BOOKS = 4
VOCAB = 2048
TEXT = 64
SEQ = 512
CLIPS = 32
TOKENS = 16384


def draw_layer_master(key, part):
    rows = 8 * D + 2 * FF
    base = jnp.clip(jax.random.normal(key, (rows, D), jnp.float32), -4.0, 4.0)
    index = jnp.arange(rows)
    scale = jnp.where(index >= 8 * D + FF, FF ** (-0.5), D ** (-0.5))
    larger = (index >= 3 * D) & (index < 4 * D) | (index >= 7 * D) & (index < 8 * D)
    scale = jnp.where(larger, 4.0 * D ** (-0.5), scale)
    return base * scale[:, None]


def draw_norm_master(key, part):
    base = jnp.clip(jax.random.normal(key, (8, D), jnp.float32), -3.0, 3.0)
    even = (jnp.arange(8) % 2 == 0)[:, None]
    return jnp.where(even, 1.0 + 0.15 * base, 0.3 * base)


def draw_table_master(key, part):
    base = jnp.clip(jax.random.normal(key, (2, BOOKS * VOCAB, D), jnp.float32), -4.0, 4.0)
    scale = jnp.array([0.5, 0.0625], jnp.float32)
    return base * scale[:, None, None]


def plant(entries, stream_key, smallest, high):
    index_at = [jax.random.randint(jax.random.fold_in(stream_key, axis), (), 0, length) for axis, length in enumerate(entries.shape)]
    widest = entries.shape.index(max(entries.shape))
    neighbour = index_at[:widest] + [(index_at[widest] + 1) % entries.shape[widest]] + index_at[widest + 1:]
    return entries.at[tuple(index_at)].set(smallest).at[tuple(neighbour)].set(high)


def steps_of(key, shape, shards, least, largest):
    def one(dim, shards_of):
        steps = jax.random.uniform(jax.random.fold_in(jax.random.fold_in(key, 6), dim), (shards_of,), jnp.float32, least / len(shards), largest / len(shards))
        return jnp.repeat(jnp.exp(steps), shape[dim] // shards_of).reshape((-1,) + (1,) * (len(shape) - dim - 1))

    factor_of = one(*shards[0])
    for cut in shards[1:]:
        factor_of = factor_of * one(*cut)
    return factor_of


def rank_table(count, skew):
    weights = [(1 << 20) // math.isqrt(rank ** skew) + 1 for rank in range(1, count + 1)]
    scale = 1 + sum(weights) // (1 << 30)
    return np.cumsum(np.array([max(1, weight // scale) for weight in weights]))


def ranked_ids(stream_key, extent, amount, slope):
    listing = rank_table(amount, slope)
    ticket = jax.random.randint(jax.random.fold_in(stream_key, 1), extent, 0, int(listing[amount - 1]))
    standing = jnp.searchsorted(jnp.asarray(listing, jnp.int32), ticket, side="right")
    return jax.random.permutation(jax.random.fold_in(stream_key, 2), amount)[standing].astype(jnp.int32)


def scatter_about(stream_key, extent, deviation, reach, shards=(), held_as=jnp.bfloat16):
    values = deviation * jax.random.normal(stream_key, extent, jnp.float32)
    if shards:
        values = values * steps_of(stream_key, extent, shards, -0.22, 0.18)
    return jnp.clip(values, -reach, reach).astype(held_as)


def setup_inputs(seed: int = 0) -> dict:
    seeds = jax.random.split(jax.random.key(seed), 16)
    return {
        "code_ids": plant(ranked_ids(seeds[0], (TOKENS, BOOKS), VOCAB, 2), jax.random.fold_in(seeds[0], 3), 0, VOCAB - 1).astype(jnp.int32),
        "target_ids": plant(ranked_ids(seeds[1], (TOKENS, BOOKS), VOCAB, 2), jax.random.fold_in(seeds[1], 3), 0, VOCAB - 1).astype(jnp.int32),
        "valid_mask": plant((jax.random.randint(seeds[2], (TOKENS, BOOKS), 0, 8) < 7).astype(jnp.int32), jax.random.fold_in(seeds[2], 1), 0, 1),
        "clip_weight": plant(jax.random.randint(seeds[3], (CLIPS,), 0, 4), jax.random.fold_in(seeds[3], 1), 0, 3).astype(jnp.int32),
        "text_states": scatter_about(seeds[4], (CLIPS * TEXT, D), 1.0, 6.0, ((0, 32),)),
        "layer_master": draw_layer_master(jax.random.fold_in(seeds[15], 71), 0),
        "layer_first": scatter_about(seeds[6], (8 * D + 2 * FF, D), (1e-5), 0.00015258789, ((0, 4),), jnp.float32),
        "layer_second": jnp.clip(jnp.exp(math.log(9.999999717180685e-10) - 2.3025851 * jax.random.uniform(seeds[7], (8 * D + 2 * FF, D), jnp.float32) ** steps_of(seeds[7], (8 * D + 2 * FF, D), ((0, 4),), -0.2, 0.2)), 1.000000013351432e-10, 9.999999717180685e-10),
        "norm_master": draw_norm_master(jax.random.fold_in(seeds[15], 71), 0),
        "norm_first": scatter_about(seeds[9], (8, D), (1e-5), 0.00015258789, ((1, 4),), jnp.float32),
        "norm_second": jnp.clip(jnp.exp(math.log(9.999999717180685e-10) - 2.3025851 * jax.random.uniform(seeds[10], (8, D), jnp.float32) ** steps_of(seeds[10], (8, D), ((1, 4),), -0.2, 0.2)), 1.000000013351432e-10, 9.999999717180685e-10),
        "table_master": draw_table_master(jax.random.fold_in(seeds[15], 71), 0),
        "table_first": scatter_about(seeds[12], (2, BOOKS * VOCAB, D), (1e-5), 0.00015258789, ((1, 32),), jnp.float32),
        "table_second": jnp.clip(jnp.exp(math.log(9.999999717180685e-10) - 2.3025851 * jax.random.uniform(seeds[13], (2, BOOKS * VOCAB, D), jnp.float32) ** steps_of(seeds[13], (2, BOOKS * VOCAB, D), ((1, 32),), -0.2, 0.2)), 1.000000013351432e-10, 9.999999717180685e-10),
        "step_count": jax.random.randint(seeds[14], (1,), 1, 21).astype(jnp.int32),
    }


@jax.custom_vjp
def low(v):
    return lax.optimization_barrier(v.astype(jnp.bfloat16)).astype(jnp.float32)

@jax.custom_vjp
def low_back(v):
    return v

def low_keep(v):
    return (low(v), None)

def low_pass(kept, grad):
    return (grad,)

def back_keep(v):
    return (v, None)

def back_low(kept, grad):
    return (low(grad),)
low.defvjp(low_keep, low_pass)
low_back.defvjp(back_keep, back_low)
norm_epsilon = 1e-05
smoothing = 0.1
zloss_weight = 0.01
clip_limit = 0.25
learn_rate = 0.05
first_decay = 0.9
second_decay = 0.95
adam_epsilon = 1e-08
weight_decay = 0.1

def matmul_high(left, right):
    return jnp.dot(left, right, precision=lax.Precision.HIGHEST, preferred_element_type=jnp.float32)

def positions(length, width):
    half = width // 2
    rates = jnp.exp(jnp.arange(half, dtype=jnp.float32) * (-math.log(10000.0) / (half - 1)))
    angles = jnp.arange(length, dtype=jnp.float32)[:, None] * rates[None, :]
    return jnp.concatenate([jnp.cos(angles), jnp.sin(angles)], axis=1)

def layer_norm(stream, gain, shift):
    mean = lax.optimization_barrier(jnp.mean(stream, axis=-1, keepdims=True))
    centred = stream - mean
    spread = lax.optimization_barrier(jnp.mean(centred * centred, axis=-1, keepdims=True))
    return centred * lax.rsqrt(spread + norm_epsilon) * gain + shift

def attend(query, keys, values, causal):
    rows = query.shape[0]
    cols = keys.shape[0]
    query_heads = query.reshape(rows, HEADS, HEAD)
    key_heads = keys.reshape(cols, HEADS, HEAD)
    value_heads = values.reshape(cols, HEADS, HEAD)
    scores = low_back(jnp.einsum('qhd,khd->hqk', query_heads, key_heads, precision=lax.Precision.HIGHEST))
    if causal:
        allowed = jnp.arange(rows)[:, None] >= jnp.arange(cols)[None, :]
        scores = jnp.where(allowed[None], scores, -1e+30)
    probs = low(jax.nn.softmax(scores, axis=-1))
    mixed = jnp.einsum('hqk,khd->qhd', probs, value_heads, precision=lax.Precision.HIGHEST)
    return low(low_back(mixed.reshape(rows, D)))

def token_losses(logits, targets, weights):
    rows = logits.shape[0]
    grouped = logits.reshape(rows, BOOKS, VOCAB)
    totals = jax.nn.logsumexp(grouped, axis=-1)
    picked = jnp.take_along_axis(grouped, targets[:, :, None], axis=-1)[:, :, 0]
    average = lax.optimization_barrier(jnp.mean(grouped, axis=-1))
    term = totals - (1.0 - smoothing) * picked - smoothing * average + zloss_weight * totals * totals
    return jnp.sum(weights * term)

def clip_loss(layer, gains, tables, codes, targets, weights, text, position_table):
    book_rows = codes + VOCAB * jnp.arange(BOOKS, dtype=jnp.int32)[None, :]
    stream_zero = lax.optimization_barrier(jnp.sum(tables[0][book_rows], axis=1)) + position_table
    scale = HEAD ** (-0.5)
    normed_one = low(layer_norm(stream_zero, gains[0], gains[1]))
    project = matmul_high(normed_one, layer[0:3 * D].T)
    query = low(low_back(project[:, 0:D] * scale))
    keys = low(low_back(project[:, D:2 * D]))
    values = low(low_back(project[:, 2 * D:3 * D]))
    self_mix = attend(query, keys, values, True)
    stream_one = stream_zero + low_back(matmul_high(self_mix, layer[3 * D:4 * D].T))
    normed_two = low(layer_norm(stream_one, gains[2], gains[3]))
    cross_query = low(low_back(matmul_high(normed_two, layer[4 * D:5 * D].T) * scale))
    text_project = matmul_high(text, layer[5 * D:7 * D].T)
    text_keys = low(low_back(text_project[:, 0:D]))
    text_values = low(low_back(text_project[:, D:2 * D]))
    cross_mix = attend(cross_query, text_keys, text_values, False)
    stream_two = stream_one + low_back(matmul_high(cross_mix, layer[7 * D:8 * D].T))
    normed_three = low(layer_norm(stream_two, gains[4], gains[5]))
    hidden_pre = low_back(matmul_high(normed_three, layer[8 * D:8 * D + FF].T))
    hidden = low(jax.nn.gelu(hidden_pre, approximate=False))
    stream_three = stream_two + low_back(matmul_high(hidden, layer[8 * D + FF:8 * D + 2 * FF]))
    normed_four = low(layer_norm(stream_three, gains[6], gains[7]))
    logits = low_back(matmul_high(normed_four, tables[1].T))
    return token_losses(logits, targets, weights)

def adam_update(master, first, second, grad, count_step):
    first_new = first_decay * first + (1.0 - first_decay) * grad
    second_new = second_decay * second + (1.0 - second_decay) * grad * grad
    first_hat = first_new / (1.0 - jnp.power(first_decay, count_step))
    second_hat = second_new / (1.0 - jnp.power(second_decay, count_step))
    master_new = master - learn_rate * (first_hat / (jnp.sqrt(second_hat) + adam_epsilon) + weight_decay * master)
    return (master_new, first_new, second_new)

def reference(code_ids, target_ids, valid_mask, clip_weight, text_states, layer_master, layer_first, layer_second, norm_master, norm_first, norm_second, table_master, table_first, table_second, step_count):
    layer_used = layer_master.astype(jnp.bfloat16).astype(jnp.float32)
    gains_used = norm_master.astype(jnp.bfloat16).astype(jnp.float32)
    tables_used = table_master.astype(jnp.bfloat16).astype(jnp.float32)
    clips = clip_weight.shape[0]
    code_blocks = code_ids.reshape(clips, SEQ, BOOKS)
    target_blocks = target_ids.reshape(clips, SEQ, BOOKS)
    weight_blocks = clip_weight.astype(jnp.float32)[:, None, None] * valid_mask.astype(jnp.float32).reshape(clips, SEQ, BOOKS)
    text_blocks = text_states.astype(jnp.float32).reshape(clips, TEXT, D)
    count = clips * SEQ * BOOKS
    position_table = positions(SEQ, D)
    checked = jax.checkpoint(clip_loss)

    def total_loss(layer, gains, tables):

        def one_clip(carry, item):
            codes, targets, weights, text = item
            return (carry + checked(layer, gains, tables, codes, targets, weights, text, position_table), None)
        summed, unused = lax.scan(one_clip, jnp.zeros((), jnp.float32), (code_blocks, target_blocks, weight_blocks, text_blocks))
        return summed / count
    loss, pullback = jax.vjp(total_loss, layer_used, gains_used, tables_used)
    grad_layer, grad_gains, grad_tables = pullback(jnp.ones((), jnp.float32))
    squares = jnp.sum(grad_layer * grad_layer) + jnp.sum(grad_gains * grad_gains) + jnp.sum(grad_tables * grad_tables)
    grad_norm = jnp.sqrt(squares)
    factor = jnp.minimum(1.0, clip_limit / grad_norm)
    count_step = step_count[0].astype(jnp.float32)
    layer_new, layer_first_new, layer_second_new = adam_update(layer_master, layer_first, layer_second, grad_layer * factor, count_step)
    norm_new, norm_first_new, norm_second_new = adam_update(norm_master, norm_first, norm_second, grad_gains * factor, count_step)
    table_new, table_first_new, table_second_new = adam_update(table_master, table_first, table_second, grad_tables * factor, count_step)
    return (loss.reshape(1), grad_norm.reshape(1), layer_new, layer_first_new, layer_second_new, norm_new, norm_first_new, norm_second_new, table_new, table_first_new, table_second_new)
```

```python
import math

import jax
import jax.numpy as jnp
from jax import lax
from jax.experimental import pallas as pl
from jax.experimental.pallas import tpu as pltpu
from jax.sharding import PartitionSpec as P

D = 1024
HEADS = 16
HEAD = 64
FF = 4096
BOOKS = 4
VOCAB = 2048
SEQ = 512

norm_epsilon = 1e-05
smoothing = 0.1
zloss_weight = 0.01
clip_limit = 0.25
learn_rate = 0.05
first_decay = 0.9
second_decay = 0.95
adam_epsilon = 1e-08
weight_decay = 0.1

F16_TOP = 32768.0
MESH = pl.DeviceIdType.MESH


def times_trans(left, right):
    return lax.dot_general(
        left, right, (((1,), (1,)), ((), ())), preferred_element_type=jnp.float32
    )


def trans_times(left, right):
    return lax.dot_general(
        left, right, (((0,), (0,)), ((), ())), preferred_element_type=jnp.float32
    )


def times_plain(left, right):
    return jnp.dot(left, right, preferred_element_type=jnp.float32)


def positions(length, width):
    half = width // 2
    rates = jnp.exp(jnp.arange(half, dtype=jnp.float32) * (-math.log(10000.0) / (half - 1)))
    angles = jnp.arange(length, dtype=jnp.float32)[:, None] * rates[None, :]
    return jnp.concatenate([jnp.cos(angles), jnp.sin(angles)], axis=1)


def layer_norm(stream, gain, shift):
    mean = jnp.mean(stream, axis=-1, keepdims=True)
    centred = stream - mean
    spread = jnp.mean(centred * centred, axis=-1, keepdims=True)
    return centred * lax.rsqrt(spread + norm_epsilon) * gain + shift


def exact_gelu(values):
    return jax.nn.gelu(values, approximate=False)


def attend_scores(query, keys, causal):
    rows = query.shape[0]
    cols = keys.shape[0]
    query_heads = query.reshape(rows, HEADS, HEAD)
    key_heads = keys.reshape(cols, HEADS, HEAD)
    scores = jnp.einsum("qhd,khd->hqk", query_heads, key_heads, preferred_element_type=jnp.float32)
    if causal:
        allowed = jnp.arange(rows)[:, None] >= jnp.arange(cols)[None, :]
        scores = jnp.where(allowed[None], scores, -1e30)
    return scores


def attend_forward(query, keys, values, causal):
    scores = attend_scores(query, keys, causal)
    totals = jax.nn.logsumexp(scores, axis=-1)
    probs = jnp.exp(scores - totals[:, :, None]).astype(jnp.bfloat16)
    value_heads = values.reshape(values.shape[0], HEADS, HEAD)
    mixed = jnp.einsum("hqk,khd->qhd", probs, value_heads, preferred_element_type=jnp.float32)
    return (mixed.reshape(query.shape[0], D).astype(jnp.bfloat16), totals)


def attend_backward(query, keys, values, totals, grad_out, causal):
    rows = query.shape[0]
    cols = keys.shape[0]
    scores = attend_scores(query, keys, causal)
    probs = jnp.exp(scores - totals[:, :, None])
    query_heads = query.reshape(rows, HEADS, HEAD)
    key_heads = keys.reshape(cols, HEADS, HEAD)
    value_heads = values.reshape(cols, HEADS, HEAD)
    grad_heads = grad_out.reshape(rows, HEADS, HEAD)
    grad_probs = jnp.einsum(
        "qhd,khd->hqk", grad_heads, value_heads, preferred_element_type=jnp.float32
    )
    grad_values = jnp.einsum(
        "hqk,qhd->khd", probs.astype(jnp.bfloat16), grad_heads, preferred_element_type=jnp.float32
    )
    grad_scores = (
        probs * (grad_probs - jnp.sum(probs * grad_probs, axis=-1, keepdims=True))
    ).astype(jnp.bfloat16)
    grad_query = jnp.einsum(
        "hqk,khd->qhd", grad_scores, key_heads, preferred_element_type=jnp.float32
    )
    grad_keys = jnp.einsum(
        "hqk,qhd->khd", grad_scores, query_heads, preferred_element_type=jnp.float32
    )
    return (grad_query.reshape(rows, D), grad_keys.reshape(cols, D), grad_values.reshape(cols, D))


def adam_update(master, first, second, grad, count_step):
    first_new = first_decay * first + (1.0 - first_decay) * grad
    second_new = second_decay * second + (1.0 - second_decay) * grad * grad
    first_hat = first_new / (1.0 - jnp.power(first_decay, count_step))
    second_hat = second_new / (1.0 - jnp.power(second_decay, count_step))
    master_new = master - learn_rate * (
        first_hat / (jnp.sqrt(second_hat) + adam_epsilon) + weight_decay * master
    )
    return (master_new, first_new, second_new)


def exchange_kernel(n_dp, n_sh, scatter, x_ref, o_ref, send_sem, recv_sem):
    n = n_dp * n_sh
    me = lax.axis_index("dp") * n_sh + lax.axis_index("shard")

    def device(k):
        t = lax.rem(me + k, n)
        return t, (t // n_sh, lax.rem(t, n_sh))

    barrier = pltpu.get_barrier_semaphore()

    def greet(k, _):
        pl.semaphore_signal(barrier, inc=1, device_id=device(k)[1], device_id_type=MESH)
        return 0

    lax.fori_loop(1, n, greet, 0)
    pl.semaphore_wait(barrier, n - 1)

    def copy(k):
        t, where = device(k)
        return pltpu.make_async_remote_copy(
            src_ref=x_ref.at[t] if scatter else x_ref,
            dst_ref=o_ref.at[me],
            send_sem=send_sem.at[k],
            recv_sem=recv_sem.at[k],
            device_id=where,
            device_id_type=MESH,
        )

    def begin(k, _):
        copy(k).start()
        return 0

    def finish(k, _):
        copy(k).wait()
        return 0

    lax.fori_loop(1, n, begin, 0)
    o_ref[me] = x_ref[me] if scatter else x_ref[...]
    lax.fori_loop(1, n, finish, 0)


def exchange(tile, n_dp, n_sh, scatter=False):
    n = n_dp * n_sh
    shape = tile.shape if scatter else (n,) + tile.shape
    return pl.pallas_call(
        lambda *refs: exchange_kernel(n_dp, n_sh, scatter, *refs),
        out_shape=jax.ShapeDtypeStruct(shape, tile.dtype),
        in_specs=[pl.BlockSpec(memory_space=pltpu.VMEM)],
        out_specs=pl.BlockSpec(memory_space=pltpu.VMEM),
        scratch_shapes=[pltpu.SemaphoreType.DMA((n,)), pltpu.SemaphoreType.DMA((n,))],
        compiler_params=pltpu.CompilerParams(
            collective_id=1 if scatter else 0, has_side_effects=True
        ),
        name="exchange_scatter" if scatter else "exchange_all",
    )(tile)


def scalar_tile(values):
    row = jnp.stack([v.reshape(()) for v in values])
    row = jnp.pad(row, (0, 128 - len(values)))
    return jnp.broadcast_to(row[None, :], (8, 128))


class Ring:
    def __init__(self):
        self.n_dp = lax.axis_size("dp")
        self.n_sh = lax.axis_size("shard")
        self.dp_bits = self.n_dp.bit_length() - 1
        self.sh_bits = self.n_sh.bit_length() - 1
        assert self.n_dp == 1 << self.dp_bits and self.n_sh == 1 << self.sh_bits
        self.index = {"d": lax.axis_index("dp"), "s": lax.axis_index("shard")}

    def bit(self, name):
        return (self.index[name[0]] >> int(name[1:])) & 1

    def swap(self, value, name):
        axis, size = ("dp", self.n_dp) if name[0] == "d" else ("shard", self.n_sh)
        flip = 1 << int(name[1:])
        return lax.ppermute(value, axis, [(i, i ^ flip) for i in range(size)])

    def dp_names(self):
        return [f"d{b}" for b in reversed(range(self.dp_bits))]

    def sh_names(self):
        return [f"s{b}" for b in reversed(range(self.sh_bits))]

    def orders(self):
        others = [f"s{b}" for b in range(1, self.sh_bits)]
        rest = [f"d{b}" for b in range(1, self.dp_bits)]
        first = ["d0"] + others + rest
        second = others + ["d0"] + rest
        return first, second

    def reduce(self, group, names):
        rows = group.shape[0] >> len(names)
        shape = (2,) * len(names) + (2, rows // 2, group.shape[1])
        full = group.reshape(shape)

        def pick(value, left, name, bit):
            return lax.dynamic_index_in_dim(value, bit, left.index(name), keepdims=False)

        def step(parts, left, name):
            mine = self.bit(name)
            send = sum(pick(p, left, name, 1 - mine).astype(jnp.float32) for p in parts)
            got = self.swap(send.astype(jnp.float16), name)
            kept = [pick(p, left, name, mine) for p in parts]
            return kept + [got], [n for n in left if n != name]

        parts, left = step([full], list(names), "s0")
        outs = []
        for half, order in enumerate(self.orders()):
            pieces, open_ = [p[..., half, :, :] for p in parts], list(left)
            for name in order:
                pieces, open_ = step(pieces, open_, name)
            outs.append(sum(p.astype(jnp.float32) for p in pieces))
        return jnp.concatenate(outs, axis=0)

    def gather_dp(self, block):
        now = block[None]
        for b in reversed(range(self.dp_bits)):
            name = f"d{b}"
            got = self.swap(now, name)
            mine = self.bit(name)
            low = jnp.where(mine == 0, now, got)
            high = jnp.where(mine == 0, got, now)
            now = jnp.stack([low, high], axis=1).reshape((-1,) + block.shape)
        return now.reshape(-1, block.shape[1])


def rowmax(value):
    return jnp.max(jnp.abs(value.astype(jnp.float32)), axis=-1)


def bound_of(left, right):
    return jnp.sum(rowmax(left) * rowmax(right))


def scale_of(bound):
    return F16_TOP / jnp.maximum(bound, 1e-30)


def to_half(value, scale):
    return (value * scale).astype(jnp.float16)


def body(
    code_ids,
    target_ids,
    valid_mask,
    clip_weight,
    text_states,
    layer_master,
    layer_first,
    layer_second,
    norm_master,
    norm_first,
    norm_second,
    table_master,
    table_first,
    table_second,
    step_count,
):
    ring = Ring()
    n_dp, n_sh = ring.n_dp, ring.n_sh
    n = n_dp * n_sh
    gains_low = lax.all_gather(norm_master.astype(jnp.bfloat16), "shard", axis=1, tiled=True)
    embed_rows = lax.all_gather(
        table_master[0].astype(jnp.bfloat16), ("dp", "shard"), axis=0, tiled=True
    )
    layer_low = lax.all_gather(layer_master.astype(jnp.bfloat16), "shard", axis=0, tiled=True)
    head_rows = lax.all_gather(
        table_master[1].astype(jnp.bfloat16), ("dp", "shard"), axis=0, tiled=True
    )
    gains = gains_low.astype(jnp.float32)
    count = float(SEQ * BOOKS * n)
    scale = HEAD ** (-0.5)

    def one_hot(codes):
        vocab = jnp.arange(VOCAB, dtype=jnp.int32)[None, :]
        return jnp.concatenate(
            [(codes[:, k : k + 1] == vocab).astype(jnp.bfloat16) for k in range(BOOKS)], axis=1
        )

    stream_zero = times_plain(one_hot(code_ids), embed_rows) + positions(SEQ, D)
    normed_one, back_one = jax.vjp(layer_norm, stream_zero, gains[0], gains[1])
    input_one = normed_one.astype(jnp.bfloat16)
    project = times_trans(input_one, layer_low[0 : 3 * D])
    query = (project[:, 0:D] * scale).astype(jnp.bfloat16)
    keys = project[:, D : 2 * D].astype(jnp.bfloat16)
    values = project[:, 2 * D : 3 * D].astype(jnp.bfloat16)
    self_mix, self_totals = attend_forward(query, keys, values, True)
    stream_one = stream_zero + times_trans(self_mix, layer_low[3 * D : 4 * D])
    normed_two, back_two = jax.vjp(layer_norm, stream_one, gains[2], gains[3])
    input_two = normed_two.astype(jnp.bfloat16)
    cross_query = (times_trans(input_two, layer_low[4 * D : 5 * D]) * scale).astype(jnp.bfloat16)
    text_project = times_trans(text_states, layer_low[5 * D : 7 * D])
    text_keys = text_project[:, 0:D].astype(jnp.bfloat16)
    text_values = text_project[:, D : 2 * D].astype(jnp.bfloat16)
    cross_mix, cross_totals = attend_forward(cross_query, text_keys, text_values, False)
    stream_two = stream_one + times_trans(cross_mix, layer_low[7 * D : 8 * D])
    normed_three, back_three = jax.vjp(layer_norm, stream_two, gains[4], gains[5])
    input_three = normed_three.astype(jnp.bfloat16)
    hidden_pre = times_trans(input_three, layer_low[8 * D : 8 * D + FF])
    hidden, back_gelu = jax.vjp(exact_gelu, hidden_pre)
    hidden_low = hidden.astype(jnp.bfloat16)
    stream_three = stream_two + times_plain(hidden_low, layer_low[8 * D + FF : 8 * D + 2 * FF])
    normed_four, back_four = jax.vjp(layer_norm, stream_three, gains[6], gains[7])
    input_four = normed_four.astype(jnp.bfloat16)

    weights = clip_weight.astype(jnp.float32)[0] * valid_mask.astype(jnp.float32)
    vocab = lax.broadcasted_iota(jnp.int32, (SEQ, VOCAB), 1)
    local_loss = jnp.zeros((), jnp.float32)
    grad_logits = []
    for k in range(BOOKS):
        logit = times_trans(input_four, head_rows[k * VOCAB : (k + 1) * VOCAB])
        top = jnp.max(logit, axis=-1, keepdims=True)
        total = top + jnp.log(jnp.sum(jnp.exp(logit - top), axis=-1, keepdims=True))
        hit = vocab == target_ids[:, k : k + 1]
        picked = jnp.sum(jnp.where(hit, logit, 0.0), axis=-1, keepdims=True)
        average = jnp.mean(logit, axis=-1, keepdims=True)
        term = (
            total - (1.0 - smoothing) * picked - smoothing * average + zloss_weight * total * total
        )
        weight = weights[:, k : k + 1]
        local_loss = local_loss + jnp.sum(weight * term)
        part = jnp.exp(logit - total) * (1.0 + 2.0 * zloss_weight * total)
        part = part - jnp.where(hit, 1.0 - smoothing, 0.0) - smoothing / VOCAB
        grad_logits.append((part * (weight / count)).astype(jnp.bfloat16))
    local_loss = local_loss / count

    max_logits = grad_logits[0]
    row_logits = rowmax(grad_logits[0])
    for k in range(1, BOOKS):
        row_logits = jnp.maximum(row_logits, rowmax(grad_logits[k]))
    bound_head = jnp.sum(row_logits * rowmax(input_four))
    seen = exchange(scalar_tile([bound_head, local_loss]), n_dp, n_sh)[:, 0, 0:2]
    seen = jnp.sum(seen, axis=0)
    loss_total = seen[1]
    scale_head = scale_of(seen[0])
    grad_four = sum(
        times_plain(grad_logits[k], head_rows[k * VOCAB : (k + 1) * VOCAB]) for k in range(BOOKS)
    )
    grad_head = jnp.concatenate(
        [to_half(trans_times(grad_logits[k], input_four), scale_head) for k in range(BOOKS)], axis=0
    )
    table_names = ring.dp_names() + ring.sh_names()
    own_head = ring.reduce(grad_head, table_names)

    grad_stream, grad_gain_four, grad_shift_four = back_four(grad_four)
    branch_three = grad_stream.astype(jnp.bfloat16)
    grad_hidden = times_trans(branch_three, layer_low[8 * D + FF : 8 * D + 2 * FF])
    grad_pre = back_gelu(grad_hidden)[0].astype(jnp.bfloat16)
    bound_ff = jnp.maximum(bound_of(hidden_low, branch_three), bound_of(grad_pre, input_three))
    scale_ff = scale_of(
        jnp.sum(exchange(scalar_tile([bound_ff]), n_dp, n_sh)[:, 0, 0])
    )
    grad_down = to_half(trans_times(hidden_low, branch_three), scale_ff)
    grad_up = to_half(trans_times(grad_pre, input_three), scale_ff)
    layer_names = ring.sh_names()[1:] + ring.dp_names() + ring.sh_names()[:1]
    own_ff = ring.reduce(jnp.concatenate([grad_up, grad_down], axis=0), layer_names)

    grad_three, grad_gain_three, grad_shift_three = back_three(
        times_plain(grad_pre, layer_low[8 * D : 8 * D + FF])
    )
    grad_stream = grad_stream + grad_three
    branch_two = grad_stream.astype(jnp.bfloat16)
    grad_cross_mix = times_plain(branch_two, layer_low[7 * D : 8 * D]).astype(jnp.bfloat16)
    grad_cross_query, grad_text_keys, grad_text_values = attend_backward(
        cross_query, text_keys, text_values, cross_totals, grad_cross_mix, False
    )
    grad_cross_low = grad_cross_query.astype(jnp.bfloat16) * scale
    grad_text = jnp.concatenate(
        [grad_text_keys.astype(jnp.bfloat16), grad_text_values.astype(jnp.bfloat16)], axis=1
    )
    grad_two, grad_gain_two, grad_shift_two = back_two(
        times_plain(grad_cross_low, layer_low[4 * D : 5 * D])
    )
    grad_stream = grad_stream + grad_two
    branch_one = grad_stream.astype(jnp.bfloat16)
    grad_self_mix = times_plain(branch_one, layer_low[3 * D : 4 * D]).astype(jnp.bfloat16)
    grad_query, grad_keys, grad_values = attend_backward(
        query, keys, values, self_totals, grad_self_mix, True
    )
    grad_project = jnp.concatenate(
        [
            grad_query.astype(jnp.bfloat16) * scale,
            grad_keys.astype(jnp.bfloat16),
            grad_values.astype(jnp.bfloat16),
        ],
        axis=1,
    )
    grad_one, grad_gain_one, grad_shift_one = back_one(
        times_plain(grad_project, layer_low[0 : 3 * D])
    )
    grad_stream = grad_stream + grad_one

    bound_mix = bound_of(branch_two, cross_mix)
    for left, right in (
        (grad_cross_low, input_two),
        (grad_text, text_states),
        (branch_one, self_mix),
        (grad_project, input_one),
    ):
        bound_mix = jnp.maximum(bound_mix, bound_of(left, right))
    bound_embed = jnp.sum(rowmax(grad_stream))
    grad_gains = jnp.stack(
        [
            grad_gain_one,
            grad_shift_one,
            grad_gain_two,
            grad_shift_two,
            grad_gain_three,
            grad_shift_three,
            grad_gain_four,
            grad_shift_four,
        ]
    )
    share = 8 * D // n
    lanes = -(-share // 128)
    slices = jnp.pad(grad_gains.reshape(n, share), ((0, 0), (0, lanes * 128 - share)))
    slices = slices.reshape(n, lanes, 128)
    bounds = jnp.broadcast_to(scalar_tile([bound_mix, bound_embed])[None, : 8 - lanes], (n, 8 - lanes, 128))
    seen = jnp.sum(
        exchange(jnp.concatenate([slices, bounds], axis=1), n_dp, n_sh, scatter=True), axis=0
    )
    own_slice = seen[:lanes]
    scale_mix, scale_embed = scale_of(seen[7, 0]), scale_of(seen[7, 1])

    grad_mix = jnp.concatenate(
        [
            to_half(trans_times(grad_project, input_one), scale_mix),
            to_half(trans_times(branch_one, self_mix), scale_mix),
            to_half(trans_times(grad_cross_low, input_two), scale_mix),
            to_half(trans_times(grad_text, text_states), scale_mix),
            to_half(trans_times(branch_two, cross_mix), scale_mix),
        ],
        axis=0,
    )
    own_mix = ring.reduce(grad_mix, layer_names)
    scaled = grad_stream * scale_embed
    high = scaled.astype(jnp.bfloat16)
    low = (scaled - high.astype(jnp.float32)).astype(jnp.bfloat16)
    grad_embed = trans_times(
        one_hot(jnp.concatenate([code_ids, code_ids], axis=0)), jnp.concatenate([high, low], axis=0)
    ).astype(jnp.float16)
    own_embed = ring.reduce(grad_embed, table_names)

    top_name = ring.sh_names()[0]
    top = ring.bit(top_name)
    keep = jnp.where(top == 1, own_ff, own_mix).astype(jnp.float16)
    give = jnp.where(top == 1, own_mix, own_ff).astype(jnp.float16)
    got = ring.swap(give, top_name)
    block = jnp.concatenate(
        [jnp.where(top == 0, keep, got), jnp.where(top == 0, got, keep)], axis=0
    )
    back_layer = 1.0 / jnp.where(top == 1, scale_ff, scale_mix)
    own_layer = ring.gather_dp(block)

    own_tables = jnp.stack([own_embed * (1.0 / scale_embed), own_head * (1.0 / scale_head)])
    block_wide = block.astype(jnp.float32) * back_layer
    squares = jnp.sum(own_tables * own_tables) + jnp.sum(block_wide * block_wide)
    tile = jnp.concatenate([own_slice, scalar_tile([squares])[: 8 - lanes]], axis=0)
    seen = exchange(tile, n_dp, n_sh)
    full_gains = seen[:, :lanes].reshape(n, lanes * 128)[:, :share].reshape(8, D)
    square_total = jnp.sum(seen[:, 7, 0]) + jnp.sum(full_gains * full_gains)
    width = D // n_sh
    own_gains = lax.dynamic_slice_in_dim(full_gains, lax.axis_index("shard") * width, width, axis=1)

    grad_norm = jnp.sqrt(square_total)
    factor = jnp.minimum(1.0, clip_limit / grad_norm)
    count_step = step_count[0].astype(jnp.float32)
    layer_new, layer_first_new, layer_second_new = adam_update(
        layer_master,
        layer_first,
        layer_second,
        own_layer.astype(jnp.float32) * back_layer * factor,
        count_step,
    )
    norm_new, norm_first_new, norm_second_new = adam_update(
        norm_master, norm_first, norm_second, own_gains * factor, count_step
    )
    table_new, table_first_new, table_second_new = adam_update(
        table_master, table_first, table_second, own_tables * factor, count_step
    )
    return (
        loss_total.reshape(1),
        grad_norm.reshape(1),
        layer_new,
        layer_first_new,
        layer_second_new,
        norm_new,
        norm_first_new,
        norm_second_new,
        table_new,
        table_first_new,
        table_second_new,
    )


def solution(mesh):
    return jax.shard_map(
        body,
        mesh=mesh,
        in_specs=(
            P(("dp", "shard"), None),
            P(("dp", "shard"), None),
            P(("dp", "shard"), None),
            P(("dp", "shard")),
            P(("dp", "shard"), None),
            P("shard", None),
            P("shard", None),
            P("shard", None),
            P(None, "shard"),
            P(None, "shard"),
            P(None, "shard"),
            P(None, ("dp", "shard"), None),
            P(None, ("dp", "shard"), None),
            P(None, ("dp", "shard"), None),
            P(),
        ),
        out_specs=(
            P(),
            P(),
            P("shard", None),
            P("shard", None),
            P("shard", None),
            P(None, "shard"),
            P(None, "shard"),
            P(None, "shard"),
            P(None, ("dp", "shard"), None),
            P(None, ("dp", "shard"), None),
            P(None, ("dp", "shard"), None),
        ),
        check_vma=False,
    )
```
